128 devices in a mesh: dp: 1, sp: 128 (over z, y, x, core).
Axes of the slice: x: 4, y: 4, z: 4, core: 2. Of those that a mesh axis runs over, the one named last changes fastest.
Arguments:
- dec_hidden: bfloat16 [1024, 2048], P(('dp', 'sp'))
- memory: bfloat16 [131072, 2048], P(('dp', 'sp'))
- mem_len: int32 [1], P('dp')
- gain_self: bfloat16 [2, 2048], replicated
- gain_cross: bfloat16 [2, 2048], replicated
- gain_mlp: bfloat16 [2, 2048], replicated
- self_q: bfloat16 [2, 2048, 2048], replicated
- self_k: bfloat16 [2, 2048, 2048], replicated
- self_v: bfloat16 [2, 2048, 2048], replicated
- self_o: bfloat16 [2, 2048, 2048], replicated
- cross_q: bfloat16 [2, 2048, 2048], replicated
- cross_k: bfloat16 [2, 2048, 128], replicated
- cross_v: bfloat16 [2, 2048, 128], replicated
- cross_o: bfloat16 [2, 2048, 2048], replicated
- mlp_gate: bfloat16 [2, 2048, 5120], replicated
- mlp_up: bfloat16 [2, 2048, 5120], replicated
- mlp_down: bfloat16 [2, 5120, 2048], replicated
Outputs:
- output: bfloat16 [1024, 2048], P(('dp', 'sp'))
All inputs are finite; a program needn't handle non-finite values.
Results may differ from the reference program's by a relative error of at most 0.0166283.
Values are sent between devices in bfloat16 or wider.
A program may use at most 1 GiB of HBM per device.

```python
import jax
import jax.numpy as jnp
from jax import lax

SHARDS = 128
TQ_DEV = 8
TM_DEV = 1024
D_MODEL = 2048
HEAD = 64
KV_HEADS = 2
FF_DIM = 5120
LAYERS = 2

TQ_LEN = TQ_DEV * SHARDS
TM_LEN = TM_DEV * SHARDS
HEADS = D_MODEL // HEAD
KV_DIM = HEAD * KV_HEADS
GROUP_SIZE = HEADS // KV_HEADS
ATT_SCALE = HEAD ** -0.5


def draw_matrix(key_mat, shape):
    return (jax.random.normal(key_mat, shape, jnp.float32) * shape[1] ** -0.5).astype(jnp.bfloat16)


def draw_gain(key_gain):
    return (1.0 + 0.3 * jax.random.normal(key_gain, (LAYERS, D_MODEL), jnp.float32)).astype(jnp.bfloat16)


def setup_inputs(seed: int = 0, part: int = 0) -> dict:
    part_key = jax.random.fold_in(jax.random.key(seed), part)
    part_keys = jax.random.split(part_key, 5)
    dec_noise = jax.random.normal(part_keys[0], (SHARDS, TQ_DEV, D_MODEL), jnp.float32)
    dec_shift = 0.8 * jax.random.normal(part_keys[1], (SHARDS, 1, D_MODEL), jnp.float32)
    mem_noise = jax.random.normal(part_keys[2], (SHARDS, TM_DEV, D_MODEL), jnp.float32)
    mem_shift = jax.random.normal(part_keys[3], (SHARDS, 1, D_MODEL), jnp.float32)
    mem_len = jax.random.randint(part_keys[4], (1,), TM_LEN // 4 + 1, 3 * TM_LEN // 4 + 1, dtype=jnp.int32)
    w_keys = jax.random.split(jax.random.key(seed + 1), 14)
    return {
        "dec_hidden": (dec_noise + dec_shift).reshape(TQ_LEN, D_MODEL).astype(jnp.bfloat16),
        "memory": (mem_noise + mem_shift).reshape(TM_LEN, D_MODEL).astype(jnp.bfloat16),
        "mem_len": mem_len,
        "gain_self": draw_gain(w_keys[0]),
        "gain_cross": draw_gain(w_keys[1]),
        "gain_mlp": draw_gain(w_keys[2]),
        "self_q": draw_matrix(w_keys[3], (LAYERS, D_MODEL, D_MODEL)),
        "self_k": draw_matrix(w_keys[4], (LAYERS, D_MODEL, D_MODEL)),
        "self_v": draw_matrix(w_keys[5], (LAYERS, D_MODEL, D_MODEL)),
        "self_o": draw_matrix(w_keys[6], (LAYERS, D_MODEL, D_MODEL)),
        "cross_q": draw_matrix(w_keys[7], (LAYERS, D_MODEL, D_MODEL)),
        "cross_k": draw_matrix(w_keys[8], (LAYERS, D_MODEL, KV_DIM)),
        "cross_v": draw_matrix(w_keys[9], (LAYERS, D_MODEL, KV_DIM)),
        "cross_o": draw_matrix(w_keys[10], (LAYERS, D_MODEL, D_MODEL)),
        "mlp_gate": draw_matrix(w_keys[11], (LAYERS, D_MODEL, FF_DIM)),
        "mlp_up": draw_matrix(w_keys[12], (LAYERS, D_MODEL, FF_DIM)),
        "mlp_down": draw_matrix(w_keys[13], (LAYERS, FF_DIM, D_MODEL)),
    }


def rms_norm(values, gain_vec):
    val32 = values.astype(jnp.float32)
    inv_rms = lax.rsqrt(jnp.mean(val32 * val32, axis=-1, keepdims=True) + 1e-6)
    return (val32 * inv_rms * gain_vec.astype(jnp.float32)).astype(jnp.bfloat16)


def project(rows, weight):
    return jnp.dot(rows, weight, preferred_element_type=jnp.float32)


def add_residual(hidden, update):
    return (hidden.astype(jnp.float32) + update).astype(jnp.bfloat16)


def head_attend(q_head, k_head, v_head, valid):
    scores = jnp.dot(q_head, k_head.T, preferred_element_type=jnp.float32) * ATT_SCALE
    scores = jnp.where(valid, scores, -1e30)
    row_max = jnp.max(scores, axis=1, keepdims=True)
    exp_vals = jnp.exp(scores - row_max)
    row_sum = jnp.sum(exp_vals, axis=1, keepdims=True)
    weighted = jnp.dot(exp_vals.astype(jnp.bfloat16), v_head, preferred_element_type=jnp.float32)
    return weighted / row_sum


def multi_head(q_rows, k_rows, v_rows, valid, group_size):
    q_len = q_rows.shape[0]
    k_len = k_rows.shape[0]
    q_heads = q_rows.reshape(q_len, HEADS, HEAD).transpose(1, 0, 2)
    k_heads = k_rows.reshape(k_len, -1, HEAD).transpose(1, 0, 2)
    v_heads = v_rows.reshape(k_len, -1, HEAD).transpose(1, 0, 2)

    def one_head(head_idx):
        kv_idx = head_idx // group_size
        return head_attend(q_heads[head_idx], k_heads[kv_idx], v_heads[kv_idx], valid)

    per_head = lax.map(one_head, jnp.arange(HEADS))
    return per_head.transpose(1, 0, 2).reshape(q_len, HEADS * HEAD).astype(jnp.bfloat16)


def reference(dec_hidden, memory, mem_len, gain_self, gain_cross, gain_mlp, self_q, self_k, self_v, self_o, cross_q, cross_k, cross_v, cross_o, mlp_gate, mlp_up, mlp_down):
    positions = jnp.arange(TQ_LEN)
    causal = positions[:, None] >= positions[None, :]
    mem_valid = (jnp.arange(TM_LEN) < mem_len[0])[None, :]

    def decoder_layer(hidden, layer_w):
        (g_self, g_cross, g_mlp, w_query, w_key, w_value, w_out, x_query, x_key, x_value, x_out, w_gate, w_up, w_down) = layer_w
        normed = rms_norm(hidden, g_self)
        q_rows = project(normed, w_query).astype(jnp.bfloat16)
        k_rows = project(normed, w_key).astype(jnp.bfloat16)
        v_rows = project(normed, w_value).astype(jnp.bfloat16)
        attn_out = multi_head(q_rows, k_rows, v_rows, causal, 1)
        hidden = add_residual(hidden, project(attn_out, w_out))
        normed = rms_norm(hidden, g_cross)
        q_rows = project(normed, x_query).astype(jnp.bfloat16)
        mem_k = project(memory, x_key).astype(jnp.bfloat16)
        mem_v = project(memory, x_value).astype(jnp.bfloat16)
        attn_out = multi_head(q_rows, mem_k, mem_v, mem_valid, GROUP_SIZE)
        hidden = add_residual(hidden, project(attn_out, x_out))
        normed = rms_norm(hidden, g_mlp)
        act_vals = (jax.nn.silu(project(normed, w_gate)) * project(normed, w_up)).astype(jnp.bfloat16)
        hidden = add_residual(hidden, project(act_vals, w_down))
        return hidden, None

    weights = (gain_self, gain_cross, gain_mlp, self_q, self_k, self_v, self_o, cross_q, cross_k, cross_v, cross_o, mlp_gate, mlp_up, mlp_down)
    return lax.scan(decoder_layer, dec_hidden, weights)[0]
```

```python
import functools

import jax
import jax.numpy as jnp
from jax import lax
from jax.experimental import pallas as pl
from jax.experimental.pallas import tpu as pltpu
from jax.sharding import PartitionSpec as P

F32, BF16 = jnp.float32, jnp.bfloat16
MESH = pl.DeviceIdType.MESH
HD = 64
EPS = 1e-6
NEG = -1e30
LOG2E = 1.4426950408889634
SCALE2 = LOG2E * HD ** -0.5
LAYERS = 2
GEOMETRY = {128: (4, 16), 16: (4, 2)}
NT = (((1,), (1,)), ((), ()))


class Geo:
    def __init__(self, n, d_model, ff, tm):
        self.nz, self.np_ = GEOMETRY[n]
        self.nb = min(3, self.nz)
        self.d, self.tm = d_model, tm
        self.half = d_model // 2
        self.npair = self.np_ // 2
        self.cols = self.np_ * 16
        self.cw = min(512, self.half)
        self.nc = self.half // self.cw
        self.nf = ff // 2 // self.cw
        self.reuse = 3 * self.nc // 2 if self.nc > 1 else 1
        self.reuse = min(self.reuse, 2)
        self.pslots = 4 * self.nc + 2 * (self.nf - self.reuse)
        self.rslots = 2 * self.nc + self.nf - self.nc


def rms(y, gain):
    inv = lax.rsqrt(jnp.mean(y * y, axis=-1, keepdims=True) + EPS)
    return (y * inv * gain.astype(F32)).astype(BF16)


def kernel(g, mem_len, y_ref, kv_ref, gs, gc, gm, wsq, wsk, wsv, wso, wcq, wco, wg, wu, wd, out_ref,
           y2, y16, h, wp, wr, qkv, a2a, zkv, osend, orecv, xs, psend, precv, qts, qrecv, kvb, kx, vx, qx, acc, rrecv,
           act, psem, rsem, ysem, a_s, a_r, z_s, z_r, o_s, o_r, p_s, p_r, q_s, q_r, kv_s, kv_r, r_s, r_r):
    NZ, NP, NB, D, TM, HALF = g.nz, g.np_, g.nb, g.d, g.tm, g.half
    NPAIR, COLS, CW, NC, NF = g.npair, g.cols, g.cw, g.nc, g.nf
    me = lax.axis_index("sp")
    c = lax.rem(me, 2)
    chip = me // 2
    j = lax.rem(chip, NP)
    z = chip // NP
    partner = me + 1 - 2 * c

    def dev(zz, jj, cc):
        return (zz * NP + jj) * 2 + cc

    def rcopy(src, dst, ss, rs, to):
        return pltpu.make_async_remote_copy(src_ref=src, dst_ref=dst, send_sem=ss, recv_sem=rs, device_id={"sp": to}, device_id_type=MESH)

    def loop(n, body):
        def step(i, carry):
            body(i)
            return carry
        lax.fori_loop(0, n, step, 0)

    col0 = pl.multiple_of(c * HALF, CW)
    colf = pl.multiple_of(c * (NF * CW), CW)

    def p_load(layer, k):
        if k < 3 * NC:
            w, base, n, slot = (wsq, wsk, wsv)[k // NC], col0, k % NC, k
        elif k < 4 * NC:
            w, base, n, slot = wcq, col0, k - 3 * NC, k
        else:
            i = k - 4 * NC
            w, base, n = (wg, wu)[i % 2], colf, i // 2
            slot = i if i < 2 * g.reuse else 4 * NC + i - 2 * g.reuse
        start = pl.multiple_of(base + n * CW, CW)
        pltpu.make_async_copy(w.at[layer, :, pl.ds(start, CW)], wp.at[slot], psem.at[slot]).start()

    def r_load(layer, k):
        if k < 2 * NC:
            w, base, n, slot = (wso, wco)[k // NC], col0, k % NC, k
        else:
            i = k - 2 * NC
            w, base, n = wd, colf, i
            slot = i if i < NC else NC + i
        start = pl.multiple_of(base + n * CW, CW)
        pltpu.make_async_copy(w.at[layer, pl.ds(start, CW), :], wr.at[slot], rsem.at[slot]).start()

    def p_wait(slot):
        pltpu.make_async_copy(wp.at[slot], wp.at[slot], psem.at[slot]).wait()

    def r_wait(slot):
        pltpu.make_async_copy(wr.at[slot], wr.at[slot], rsem.at[slot]).wait()

    GU = 4 * NC
    DN = 2 * NC
    for k in range(3 * NC):
        p_load(0, k)
    for k in range(NC):
        r_load(0, k)
    for k in range(3 * NC, 4 * NC):
        p_load(0, k)
    for k in range(NC, 2 * NC):
        r_load(0, k)

    barrier = pltpu.get_barrier_semaphore()

    def tell(to):
        pl.semaphore_signal(barrier, inc=1, device_id={"sp": to}, device_id_type=MESH)

    tell(partner)
    loop(NP - 1, lambda o: tell(dev(z, lax.rem(j + 1 + o, NP), c)))
    for dz in range(1, NZ):
        for cc in range(2):
            tell(dev(lax.rem(z + dz, NZ), j, cc))
    pl.semaphore_wait(barrier, 1 + (NP - 1) + 2 * (NZ - 1))

    y2[c] = y_ref[...]
    swap = rcopy(y_ref, y2.at[c], ysem.at[0], ysem.at[1], partner)
    swap.start()

    def kv_copy(layer, cc, zz):
        return rcopy(kv_ref.at[layer, cc], kvb.at[layer, z, c], kv_s.at[layer, cc, zz], kv_r.at[layer, z, c], dev(zz, j, cc))

    def kv_local(layer):
        return pltpu.make_async_copy(kv_ref.at[layer, c], kvb.at[layer, z, c], kv_r.at[layer, z, c])

    def kv_send(layer):
        @pl.when(z < NB)
        def _():
            kv_local(layer).start()
            kv_copy(layer, 1 - c, z).start()
            for dz in (NZ - 1, 1, *range(2, NZ - 1)):
                for cc in range(2):
                    kv_copy(layer, cc, lax.rem(z + dz, NZ)).start()

    def kv_sent(layer):
        @pl.when(z < NB)
        def _():
            kv_copy(layer, 1 - c, z).wait_send()
            for dz in range(1, NZ):
                for cc in range(2):
                    kv_copy(layer, cc, lax.rem(z + dz, NZ)).wait_send()

    def kv_wait(layer, blk):
        for src in range(2):
            ref = kvb.at[layer, blk, src]
            pltpu.make_async_copy(ref, ref, kv_r.at[layer, blk, src]).wait()

    kv_send(0)
    for i in range(2 * g.reuse, 2 * NF):
        p_load(0, GU + i)
    for i in range(NC, NF):
        r_load(0, DN + i)

    swap.wait()
    y16[...] = jnp.concatenate([y2[0].astype(F32), y2[1].astype(F32)], axis=0).astype(BF16)

    lane = lax.broadcasted_iota(jnp.int32, (COLS, 128), 1)
    mine = (lane >= 64) == (lax.rem(j, 2) == 1)

    def share(e, total):
        psend[...] = total
        s = rcopy(psend, precv.at[e], p_s, p_r.at[e], partner)
        s.start()
        s.wait()
        y16[...] = (y16[...].astype(F32) + (psend[...] + precv[e])).astype(BF16)

    def row_split(first, n, x_of):
        def step(i, total):
            r_wait(first + i)
            return total + jnp.dot(x_of(i), wr[first + i], preferred_element_type=F32)
        return lax.fori_loop(0, n, step, jnp.zeros((16, D), F32))

    def layer(l, carry):
        h[...] = rms(y16[...].astype(F32), gs[l])

        def project(i):
            p_wait(i)
            r = jnp.dot(h[...], wp[i], preferred_element_type=F32).astype(BF16)
            for u in range(CW // 128):
                qkv[i // NC, lax.rem(i, NC) * (CW // 128) + u] = r[:, 128 * u:128 * u + 128]
        loop(3 * NC, project)

        def a_copy(o):
            to = lax.rem(j + o, NP)
            return rcopy(qkv.at[:, to // 2], a2a.at[l, j], a_s.at[o], a_r.at[l, j], dev(z, to, c))

        loop(NP - 1, lambda o: a_copy(o + 1).start())
        a2a[l, j] = qkv[:, j // 2]
        for i in range(2 * g.reuse):
            p_load(l, GU + i)

        @pl.when(l == 0)
        def _():
            for k in range(2 * g.reuse, 3 * NC):
                p_load(1, k)

        def a_wait(o):
            i = lax.rem(j + o + 1, NP)
            ref = a2a.at[l, i]
            pltpu.make_async_copy(ref, ref, a_r.at[l, i]).wait()
        loop(NP - 1, a_wait)

        q = a2a[l, :, 0].reshape(COLS, 128)
        k = a2a[l, :, 1].reshape(COLS, 128).astype(F32)
        v = a2a[l, :, 2].reshape(COLS, 128).astype(F32)
        qm = jnp.where(mine, q.astype(F32), 0.0).astype(BF16)
        zkv[l, z] = jnp.where(mine, k, pltpu.roll(v, 64, 1)).astype(BF16)

        def z_copy(dz):
            return rcopy(zkv.at[l, z], zkv.at[l, z], z_s.at[dz], z_r.at[l, z], dev(lax.rem(z + dz, NZ), j, c))

        for dz in range(1, NZ):
            z_copy(dz).start()
        for dz in range(1, NZ):
            zz = lax.rem(z + dz, NZ)
            ref = zkv.at[l, zz]
            pltpu.make_async_copy(ref, ref, z_r.at[l, zz]).wait()

        row = z * COLS + lax.broadcasted_iota(jnp.int32, (COLS, COLS), 0)
        col = lax.broadcasted_iota(jnp.int32, (COLS, COLS), 1)
        scores = []
        for zz in range(NZ):
            s = lax.dot_general(qm, zkv[l, zz], NT, preferred_element_type=F32) * SCALE2
            scores.append(jnp.where(zz * COLS + col <= row, s, NEG))
        top = functools.reduce(jnp.maximum, [jnp.max(s, axis=1, keepdims=True) for s in scores])
        den = jnp.zeros((COLS, 1), F32)
        num = jnp.zeros((COLS, 128), F32)
        for zz in range(NZ):
            e = jnp.exp2(scores[zz] - top)
            den = den + jnp.sum(e, axis=1, keepdims=True)
            num = num + jnp.dot(e.astype(BF16), zkv[l, zz], preferred_element_type=F32)
        o_all = pltpu.roll(jnp.where(mine, 0.0, num / den), 64, 1).astype(BF16)
        osend[...] = o_all.reshape(NP, 16, 128)

        def o_copy(o):
            to = lax.rem(j + o, NP)
            return rcopy(osend.at[to], orecv.at[l, j], o_s.at[o], o_r.at[l, j], dev(z, to, c))

        loop(NP - 1, lambda o: o_copy(o + 1).start())
        orecv[l, j] = osend[j]
        loop(NP - 1, lambda o: a_copy(o + 1).wait_send())
        for dz in range(1, NZ):
            z_copy(dz).wait_send()

        def o_wait(o):
            i = lax.rem(j + o + 1, NP)
            ref = orecv.at[l, i]
            pltpu.make_async_copy(ref, ref, o_r.at[l, i]).wait()
        loop(NP - 1, o_wait)
        for u in range(NPAIR):
            pair = orecv[l, 2 * u].astype(F32) + orecv[l, 2 * u + 1].astype(F32)
            xs[128 * u // CW, :, 128 * u % CW:128 * u % CW + 128] = pair.astype(BF16)
        total = row_split(0, NC, lambda i: xs[i])
        for i in range(NC):
            r_load(l, DN + i)
        loop(NP - 1, lambda o: o_copy(o + 1).wait_send())
        share(l * 3, total)

        h[...] = rms(y16[...].astype(F32), gc[l])
        stack = []
        for i in range(NC):
            p_wait(3 * NC + i)
            r = jnp.dot(h[...], wp[3 * NC + i], preferred_element_type=F32).astype(BF16).astype(F32)
            stack += [r[:, 128 * u:128 * u + 128] for u in range(CW // 128)]
        turned = jnp.concatenate(stack, axis=0).T
        qts[...] = jnp.concatenate([turned[:64], turned[64:]], axis=1).astype(BF16)

        def q_copy(o):
            to = lax.rem(j + NP - o, NP)
            return rcopy(qts, qrecv.at[l, j], q_s.at[o], q_r.at[l, j], dev(z, to, c))

        loop(NP - 1, lambda o: q_copy(o + 1).start())
        qrecv[l, j] = qts[...]

        @pl.when(l == 0)
        def _():
            for k in range(3 * NC, 4 * NC):
                p_load(1, k)
            kv_send(1)

        first = jnp.where(z < NB, z, 0)
        lane2 = lax.broadcasted_iota(jnp.int32, (TM // 2, 128), 1)
        rows2 = lax.broadcasted_iota(jnp.int32, (TM // 2, 128), 0)

        def spread(blk, src):
            x = kvb[l, blk, src, 0:TM // 2, :].astype(F32)
            xr = pltpu.roll(x, 64, 1)
            for part, (lo, hi) in enumerate(((x, xr), (xr, x))):
                at = src * TM + part * (TM // 2)
                pos = dev(blk, j, src) * TM + part * (TM // 2) + rows2
                bias = jnp.where((lane2 == 64) & (pos >= mem_len[0]), NEG, 0.0)
                kx[blk, at:at + TM // 2, 0:128] = jnp.where(lane2 < 64, lo, hi).astype(BF16)
                kx[blk, at:at + TM // 2, 128:256] = jnp.where(lane2 < 64, lo, bias).astype(BF16)
            for u in range(TM // 128):
                vx[blk, :, src * TM + 128 * u:src * TM + 128 * u + 128] = kvb[l, blk, src, TM // 2 + 64 * u:TM // 2 + 64 * u + 64, :]

        one = jnp.where(lax.broadcasted_iota(jnp.int32, (64, COLS), 0) == 0, 1.0, 0.0).astype(BF16)

        def q_spread(i):
            x = qrecv[l, i].astype(F32) * SCALE2
            hi = x.astype(BF16)
            x = x - hi.astype(F32)
            mid = x.astype(BF16)
            low = (x - mid.astype(F32)).astype(BF16)
            qx[i] = jnp.concatenate([hi, mid, low, one], axis=0)

        def attend(blk, i, num, top, den):
            s = jnp.dot(kx[blk], qx[i], preferred_element_type=F32)
            new = jnp.max(s, axis=0, keepdims=True)
            if top is not None:
                new = jnp.maximum(new, top)
            e = jnp.exp2(s - new)
            add = jnp.sum(e, axis=0, keepdims=True)
            out = jnp.dot(vx[blk], e.astype(BF16), preferred_element_type=F32)
            if top is None:
                return out, new, add
            old = jnp.exp2(top - new)
            return num * old + out, new, den * old + add

        kv_wait(l, first)
        for src in range(2):
            spread(first, src)

        def pass1(o):
            i = lax.rem(j + o + 1, NP)

            @pl.when(o < NP - 1)
            def _():
                ref = qrecv.at[l, i]
                pltpu.make_async_copy(ref, ref, q_r.at[l, i]).wait()
            q_spread(i)
            num, top, den = attend(first, i, None, None, None)
            acc[i, 0:64] = num
            acc[i, 64:65] = top
            acc[i, 65:66] = den
        loop(NP, pass1)

        for b in range(1, NB):
            blk = lax.rem(first + b, NB)
            kv_wait(l, blk)
            for src in range(2):
                spread(blk, src)

        def r_copy(o):
            to = lax.rem(j + o, NP)
            return rcopy(acc.at[to], rrecv.at[l, j], r_s.at[o], r_r.at[l, j], dev(z, to, c))

        def pass2(o):
            i = lax.rem(j + o + 1, NP)
            num, top, den = acc[i, 0:64], acc[i, 64:65], acc[i, 65:66]
            for b in range(1, NB):
                num, top, den = attend(lax.rem(first + b, NB), i, num, top, den)
            acc[i, 0:64] = num
            acc[i, 64:65] = top
            acc[i, 65:66] = den

            @pl.when(o < NP - 1)
            def _():
                r_copy(o + 1).start()
        loop(NP, pass2)
        rrecv[l, j] = acc[j]
        loop(NP - 1, lambda o: q_copy(o + 1).wait_send())

        def r_wait2(o):
            i = lax.rem(j + o + 1, NP)
            ref = rrecv.at[l, i]
            pltpu.make_async_copy(ref, ref, r_r.at[l, i]).wait()
        loop(NP - 1, r_wait2)
        top = functools.reduce(jnp.maximum, [rrecv[l, i, 64:65] for i in range(NP)])
        num = jnp.zeros((64, COLS), F32)
        den = jnp.zeros((1, COLS), F32)
        for i in range(NP):
            w = jnp.exp2(rrecv[l, i, 64:65] - top)
            num = num + rrecv[l, i, 0:64] * w
            den = den + rrecv[l, i, 65:66] * w
        o_all = num / den
        turned = jnp.concatenate([o_all[:, :COLS // 2], o_all[:, COLS // 2:]], axis=0).T.astype(BF16)
        for u in range(NPAIR):
            xs[128 * u // CW, :, 128 * u % CW:128 * u % CW + 128] = turned[16 * u:16 * u + 16]
        loop(NP - 1, lambda o: r_copy(o + 1).wait_send())
        total = row_split(NC, NC, lambda i: xs[i])

        @pl.when(l == 0)
        def _():
            for k in range(NC, 2 * NC):
                r_load(1, k)
        share(l * 3 + 1, total)

        h[...] = rms(y16[...].astype(F32), gm[l])

        def gate_up(i):
            slot = jnp.where(i < g.reuse, 2 * i, 4 * NC + 2 * (i - g.reuse))
            p_wait(slot)
            p_wait(slot + 1)
            a = jnp.dot(h[...], wp[slot], preferred_element_type=F32)
            b = jnp.dot(h[...], wp[slot + 1], preferred_element_type=F32)
            act[i] = (a / (1.0 + jnp.exp(-a)) * b).astype(BF16)

            @pl.when((i == g.reuse - 1) & (l == 0))
            def _():
                for k in range(2 * g.reuse):
                    p_load(1, k)
        loop(NF, gate_up)

        @pl.when(l == 0)
        def _():
            for i in range(2 * g.reuse, 2 * NF):
                p_load(1, GU + i)

        def down(i, total):
            slot = jnp.where(i < NC, i, NC + i)
            r_wait(slot)
            return total + jnp.dot(act[i], wr[slot], preferred_element_type=F32)
        total = lax.fori_loop(0, NF, down, jnp.zeros((16, D), F32))

        @pl.when(l == 0)
        def _():
            for k in range(NC):
                r_load(1, k)
            for i in range(NC, NF):
                r_load(1, DN + i)
        share(l * 3 + 2, total)
        return carry

    lax.fori_loop(0, LAYERS, layer, 0)
    kv_sent(0)
    kv_sent(1)
    y = y16[...].astype(F32)
    out_ref[...] = jnp.where(c == 0, y[0:8], y[8:16]).astype(BF16)


def solution(mesh):
    n = mesh.shape["sp"]
    row_spec = P(("dp", "sp"), None)

    def device_fn(dec_hidden, memory, mem_len, gain_self, gain_cross, gain_mlp, self_q, self_k, self_v, self_o, cross_q, cross_k, cross_v, cross_o, mlp_gate, mlp_up, mlp_down):
        tm, d_model = memory.shape
        g = Geo(n, d_model, mlp_gate.shape[-1], tm)
        NP, NZ, NB, COLS, CW, NC, NF, D = g.np_, g.nz, g.nb, g.cols, g.cw, g.nc, g.nf, g.d
        keys = jnp.einsum("md,ldk->lmk", memory, cross_k, preferred_element_type=F32).astype(BF16)
        vals = jnp.einsum("md,ldk->lkm", memory, cross_v, preferred_element_type=F32).astype(BF16)
        keys = keys.reshape(LAYERS, 2, tm // 2, 2, HD).transpose(0, 3, 2, 1, 4).reshape(LAYERS, 2, tm // 2, 2 * HD)
        vals = vals.reshape(LAYERS, 2, HD, tm // 128, 128).transpose(0, 1, 3, 2, 4).reshape(LAYERS, 2, tm // 2, 128)
        kv = jnp.concatenate([keys, vals], axis=2)

        vmem = pl.BlockSpec(memory_space=pltpu.VMEM)
        hbm = pl.BlockSpec(memory_space=pl.ANY)
        dma = pltpu.SemaphoreType.DMA
        scratch = [
            pltpu.VMEM((2, 8, D), BF16),
            pltpu.VMEM((16, D), BF16),
            pltpu.VMEM((16, D), BF16),
            pltpu.VMEM((g.pslots, D, CW), BF16),
            pltpu.VMEM((g.rslots, CW, D), BF16),
            pltpu.VMEM((3, g.npair, 16, 128), BF16),
            pltpu.VMEM((LAYERS, NP, 3, 16, 128), BF16),
            pltpu.VMEM((LAYERS, NZ, COLS, 128), BF16),
            pltpu.VMEM((NP, 16, 128), BF16),
            pltpu.VMEM((LAYERS, NP, 16, 128), BF16),
            pltpu.VMEM((NC, 16, CW), BF16),
            pltpu.VMEM((16, D), F32),
            pltpu.VMEM((3 * LAYERS, 16, D), F32),
            pltpu.VMEM((64, COLS), BF16),
            pltpu.VMEM((LAYERS, NP, 64, COLS), BF16),
            pltpu.VMEM((LAYERS, NB, 2, tm, 128), BF16),
            pltpu.VMEM((NB, 2 * tm, 256), BF16),
            pltpu.VMEM((NB, 64, 2 * tm), BF16),
            pltpu.VMEM((NP, 256, COLS), BF16),
            pltpu.VMEM((NP, 72, COLS), F32),
            pltpu.VMEM((LAYERS, NP, 72, COLS), F32),
            pltpu.VMEM((NF, 16, CW), BF16),
            dma((g.pslots,)), dma((g.rslots,)), dma((2,)),
            dma((NP,)), dma((LAYERS, NP)),
            dma((NZ,)), dma((LAYERS, NZ)),
            dma((NP,)), dma((LAYERS, NP)),
            dma(()), dma((3 * LAYERS,)),
            dma((NP,)), dma((LAYERS, NP)),
            dma((LAYERS, 2, NZ)), dma((LAYERS, NB, 2)),
            dma((NP,)), dma((LAYERS, NP)),
        ]
        return pl.pallas_call(
            functools.partial(kernel, g),
            out_shape=jax.ShapeDtypeStruct(dec_hidden.shape, BF16),
            in_specs=[pl.BlockSpec(memory_space=pltpu.SMEM), vmem, hbm, vmem, vmem, vmem] + [hbm] * 9,
            out_specs=vmem,
            scratch_shapes=scratch,
            compiler_params=pltpu.CompilerParams(collective_id=0, has_side_effects=True, vmem_limit_bytes=67043328),
            name="decoder",
        )(mem_len, dec_hidden, kv, *[x.reshape(LAYERS, 1, D) for x in (gain_self, gain_cross, gain_mlp)], self_q, self_k, self_v, self_o, cross_q, cross_o, mlp_gate, mlp_up, mlp_down)

    return jax.shard_map(device_fn, mesh=mesh, in_specs=(row_spec, row_spec, P("dp")) + (P(),) * 14, out_specs=row_spec, check_vma=False)
```

```python
import functools

import jax
import jax.numpy as jnp
from jax import lax
from jax.experimental import pallas as pl
from jax.experimental.pallas import tpu as pltpu
from jax.sharding import PartitionSpec as P

F32, BF16 = jnp.float32, jnp.bfloat16
MESH = pl.DeviceIdType.MESH
HD = 64
EPS = 1e-6
NEG = -1e30
LOG2E = 1.4426950408889634
SCALE2 = LOG2E * HD ** -0.5
LAYERS = 2
NBUF, LAG = 4, 3
FLAGS = {}
GEOMETRY = {128: (4, 16), 32: (4, 4), 16: (4, 2)}
NT = (((1,), (1,)), ((), ()))


RELAYS = {
    2: ((3, 0, 2, (0, 1)), (2, 1, 3, (0, 1))),
    3: ((3, 0, 2, (0, 1)), (3, 2, 0, (0, 1)), (2, 1, 3, (0,)), (0, 1, 3, (1,))),
}


class Geo:
    def __init__(self, n, d_model, ff, tm, nb):
        self.nz, self.np_ = GEOMETRY[n]
        self.nb = nb
        self.d, self.tm = d_model, tm
        self.half = d_model // 2
        self.npair = self.np_ // 2
        self.cols = self.np_ * 16
        self.nx = 4 if self.np_ == 16 else 2
        self.ch = tm // 2
        self.cw = min(512, self.half)
        self.nc = self.half // self.cw
        self.nf = ff // 2 // self.cw
        self.reuse = 3 * self.nc // 2 if self.nc > 1 else 1
        self.reuse = min(self.reuse, 2)
        self.pslots = 4 * self.nc + 2 * (self.nf - self.reuse)
        self.rslots = 2 * self.nc + self.nf - self.nc


def rms(y, gain):
    inv = lax.rsqrt(jnp.mean(y * y, axis=-1, keepdims=True) + EPS)
    return (y * inv * gain).astype(BF16)


def kernel(g, len_ref, y_ref, mem_ref, wck, wcv, gs, gc, gm, wsq, wsk, wsv, wso, wcq, wco, wg, wu, wd, out_ref,
           mem_len, y2, y16, h, gains, wp, wr, kvsend, qsend, qa, zkv, osend, orecv, xs, psend, precv, qts, qrecv, kvs, kvb, kx, vx, qxa, qxb, acc, rrecv,
           act, s0, s1, s2, s3, m0, m1, m2, m3, psem, rsem, ysem, ak_s, ak_r, aq_s, aq_r, z_s, z_r, o_s, o_r, p_s, p_r, q_s, q_r,
           kv_s, kv_r, f_s, r_s, r_r, m_sem):
    NZ, NP, NB, D, TM, HALF = g.nz, g.np_, g.nb, g.d, g.tm, g.half
    NPAIR, COLS, CW, NC, NF = g.npair, g.cols, g.cw, g.nc, g.nf
    HC = COLS // 2
    sbuf, mbuf = (s0, s1, s2, s3), (m0, m1, m2, m3)
    me = lax.axis_index("sp")
    c = lax.rem(me, 2)
    chip = me // 2
    j = lax.rem(chip, NP)
    z = chip // NP
    partner = me + 1 - 2 * c
    NX = g.nx
    NY = NP // NX
    jx, jy = lax.rem(j, NX), j // NX

    def hops(n, size):
        return min(n, size - n)

    offsets = sorted(range(1, NP), key=lambda o: -hops(o % NX, NX) - hops(o // NX, NY))
    order = (1, 3, 4, 10, 6, 9, 11, 14, 2, 5, 7, 8, 13, 15, 12) if NP == 16 else offsets
    turns = 1 - 2 * c

    def ahead(o):
        return lax.rem(jy + NY + turns * (o // NX), NY) * NX + lax.rem(jx + NX + turns * lax.rem(o, NX), NX)

    def offset_of(o):
        return sum(jnp.where(o == n, off, 0) for n, off in enumerate(order))

    def wait_bytes(ref, sem):
        pltpu.make_async_copy(ref, ref, sem).wait()

    def dev(zz, jj, cc):
        return (zz * NP + jj) * 2 + cc

    def rcopy(src, dst, ss, rs, to):
        return pltpu.make_async_remote_copy(src_ref=src, dst_ref=dst, send_sem=ss, recv_sem=rs, device_id={"sp": to}, device_id_type=MESH)

    def loop(n, body):
        def step(i, carry):
            body(i)
            return carry
        lax.fori_loop(0, n, step, 0)

    col0 = pl.multiple_of(c * HALF, CW)
    colf = pl.multiple_of(c * (NF * CW), CW)

    def p_load(layer, k):
        if k < 3 * NC:
            w, base, n, slot = (wsk, wsv, wsq)[k // NC], col0, k % NC, k
        elif k < 4 * NC:
            w, base, n, slot = wcq, col0, k - 3 * NC, k
        else:
            i = k - 4 * NC
            w, base, n = (wg, wu)[i % 2], colf, i // 2
            slot = i if i < 2 * g.reuse else 4 * NC + i - 2 * g.reuse
        start = pl.multiple_of(base + n * CW, CW)
        pltpu.make_async_copy(w.at[layer, :, pl.ds(start, CW)], wp.at[slot], psem.at[slot]).start()

    def r_load(layer, k):
        if k < 2 * NC:
            w, base, n, slot = (wso, wco)[k // NC], col0, k % NC, k
        else:
            i = k - 2 * NC
            w, base, n = wd, colf, i
            slot = i if i < NC else NC + i
        start = pl.multiple_of(base + n * CW, CW)
        pltpu.make_async_copy(w.at[layer, pl.ds(start, CW), :], wr.at[slot], rsem.at[slot]).start()

    def p_wait(slot):
        pltpu.make_async_copy(wp.at[slot], wp.at[slot], psem.at[slot]).wait()

    def r_wait(slot):
        pltpu.make_async_copy(wr.at[slot], wr.at[slot], rsem.at[slot]).wait()

    GU = 4 * NC
    DN = 2 * NC

    MR = 2 * NC
    MW = 4 * NC
    MC = D // CW

    y_in = pltpu.make_async_copy(y_ref, y2.at[c], ysem.at[2])
    y_in.start()
    len_in = pltpu.make_async_copy(len_ref, mem_len, ysem.at[4])
    len_in.start()
    for i, ref in enumerate((gs, gc, gm)):
        pltpu.make_async_copy(ref, gains.at[i], ysem.at[3]).start()

    RB = min(256, TM // 2)
    GROUPS = TM // 2 // RB

    def w_load(n):
        for i, w in enumerate((wck, wcv)):
            at = (2 * n + i) * 128
            pltpu.make_async_copy(w.at[n], wp.at[MW + at // CW, :, pl.ds(at % CW, 128)], m_sem.at[GROUPS + n]).start()

    w_load(0)
    for r in range(GROUPS):
        for part in range(2):
            row = part * (TM // 2) + r * RB
            pltpu.make_async_copy(mem_ref.at[pl.ds(row, RB), :], wr.at[MR + row // CW, pl.ds(row % CW, RB), :], m_sem.at[r]).start()
    w_load(1)

    barrier = pltpu.get_barrier_semaphore()

    def tell(to):
        pl.semaphore_signal(barrier, inc=1, device_id={"sp": to}, device_id_type=MESH)

    tell(partner)
    loop(NP - 1, lambda o: tell(dev(z, lax.rem(j + 1 + o, NP), 1 - c)))
    for dz in range(1, NZ):
        for cc in range(2):
            tell(dev(lax.rem(z + dz, NZ), j, cc))


    for k in range(3 * NC):
        p_load(0, k)
    for k in range(NC):
        r_load(0, k)
    for k in range(3 * NC, 4 * NC):
        p_load(0, k)
    for k in range(NC, 2 * NC):
        r_load(0, k)

    lane_m = lax.broadcasted_iota(jnp.int32, (RB, 128), 1)
    WS = min(256, CW)

    def keys_values(n, r):
        def product(at):
            rows = [wr[MR + at // CW, at % CW:at % CW + RB, i * CW:i * CW + CW] for i in range(MC)]
            groups = []
            for w in range(256 * n, 256 * n + 256, WS):
                groups.append(sum(jnp.dot(rows[i], wp[MW + w // CW, i * CW:i * CW + CW, w % CW:w % CW + WS], preferred_element_type=F32) for i in range(MC)))
            return jnp.concatenate(groups, axis=1)
        at = r * RB
        lo, hi = product(at), product(TM // 2 + at)
        a, b = lo[:, :128], hi[:, :128]
        kvs[n, 0, pl.ds(at, RB), :] = jnp.where(lane_m < 64, a, pltpu.roll(b, 64, 1)).astype(BF16)
        kvs[n, 1, pl.ds(at, RB), :] = jnp.where(lane_m < 64, pltpu.roll(a, 64, 1), b).astype(BF16)
        for part, x in enumerate((lo, hi)):
            for u in range(RB // 128):
                v = x[128 * u:128 * u + 128, 128:256].T.astype(BF16)
                to = TM // 2 + (part * (TM // 256) + r * (RB // 128) + u) * 64
                for hh in range(2):
                    kvs[n, hh, pl.ds(to, 64), :] = v[64 * hh:64 * hh + 64]

    def w_wait(n):
        wait_bytes(wp.at[MW, :, pl.ds(0, 256)] if CW >= 256 else wp.at[pl.ds(MW, 256 // CW)], m_sem.at[GROUPS + n])

    def memory_group(r):
        with jax.named_scope("m_wait"):
            wait_bytes(wr.at[MR, pl.ds(0, 2 * RB)] if 2 * RB <= CW else wr.at[pl.ds(MR, 2 * RB // CW)], m_sem.at[r])
        with jax.named_scope("kv"):
            keys_values(0, r)

    w_wait(0)
    for r in range(GROUPS):
        memory_group(r)

    def half_of(ref, half):
        return ref.at[pl.ds(half * (TM // 2), TM // 2)]

    def kv_copy(layer, n, half, cc, zz):
        src, dst = half_of(kvs.at[layer, 1 - cc], half), half_of(kvb.at[layer, z, c], half)
        return rcopy(src, dst, kv_s.at[layer, n, half], kv_r.at[layer, z, c, half], dev(zz, j, cc))

    def kv_local(layer, half):
        return pltpu.make_async_copy(half_of(kvs.at[layer, 1 - c], half), half_of(kvb.at[layer, z, c], half), kv_r.at[layer, z, c, half])

    sides = (NZ - 1, 1)

    def kv_send(layer, stage):
        @pl.when(z < NB)
        def _():
            for half in ((0, 1) if stage == 0 else (stage - 1,)):
                if stage == 0:
                    kv_local(layer, half).start()
                    kv_copy(layer, 0, half, 1 - c, z).start()
                for n, dz in enumerate(sides):
                    cc = c if stage == 0 else 1 - c
                    kv_copy(layer, 1 + 2 * (stage > 0) + n, half, cc, lax.rem(z + dz, NZ)).start()

    def kv_sent(layer):
        @pl.when(z < NB)
        def _():
            for n in range(5):
                for half in range(2):
                    wait_bytes(half_of(kvs.at[layer, 0], half), kv_s.at[layer, n, half])

    relays = RELAYS[NB]

    def kv_arrive(layer, blk, src, half):
        wait_bytes(half_of(kvb.at[layer, blk, src], half), kv_r.at[layer, blk, src, half])

    def source(turn):
        return c if turn == 0 else 1 - c

    def forward(layer, n, turn, half):
        _, blk, to, _ = relays[n]
        ref = half_of(kvb.at[layer, blk, source(turn)], half)
        return rcopy(ref, ref, f_s.at[layer, n % 2, turn, half], kv_r.at[layer, blk, source(turn), half], dev(to, j, c))

    def kv_relay(layer, turn, half):
        for n, (at, blk, _, turns) in enumerate(relays):
            if turn in turns:
                @pl.when(z == at)
                def _():
                    kv_arrive(layer, blk, source(turn), half)
                    forward(layer, n, turn, half).start()

    def kv_relayed(layer):
        for n, (at, _, _, turns) in enumerate(relays):
            @pl.when(z == at)
            def _():
                for turn in turns:
                    for half in range(2):
                        forward(layer, n, turn, half).wait_send()

    def kv_wait(layer):
        for blk in range(NB):
            for turn in range(2):
                here = functools.reduce(jnp.logical_and, [z != at for at, b, _, turns in relays if b == blk and turn in turns], z >= 0)

                @pl.when(here)
                def _():
                    for half in range(2):
                        kv_arrive(layer, blk, source(turn), half)

    y_in.wait()
    with jax.named_scope("barrier"):
        pl.semaphore_wait(barrier, 1 + (NP - 1) + 2 * (NZ - 1))
    swap = rcopy(y2.at[c], y2.at[c], ysem.at[0], ysem.at[1], partner)
    swap.start()
    kv_send(0, 0)
    wait_bytes(gains, ysem.at[3])
    len_in.wait()
    with jax.named_scope("swap"):
        swap.wait()
    y16[...] = jnp.concatenate([y2[0].astype(F32), y2[1].astype(F32)], axis=0).astype(BF16)

    lane = lax.broadcasted_iota(jnp.int32, (COLS, 128), 1)
    mine = (lane >= 64) == (lax.rem(j, 2) == 1)

    lane2 = lax.broadcasted_iota(jnp.int32, (TM // 2, 128), 1)
    rows2 = lax.broadcasted_iota(jnp.int32, (TM // 2, 128), 0)

    def spread(layer, blk):
        for src in range(2):
            x = kvb[layer, blk, src, 0:TM // 2, :].astype(F32)
            xr = pltpu.roll(x, 64, 1)
            for part, (lo, hi) in enumerate(((x, xr), (xr, x))):
                at = src * TM + part * (TM // 2)
                pos = dev(blk, j, src) * TM + part * (TM // 2) + rows2
                bias = jnp.where((lane2 == 64) & (pos >= mem_len[0]), NEG, 0.0)
                kx[blk, at:at + TM // 2, 0:128] = jnp.where(lane2 < 64, lo, hi).astype(BF16)
                kx[blk, at:at + TM // 2, 128:256] = jnp.where(lane2 < 64, lo, bias).astype(BF16)
            for u in range(TM // 128):
                vx[blk, :, src * TM + 128 * u:src * TM + 128 * u + 128] = kvb[layer, blk, src, TM // 2 + 64 * u:TM // 2 + 64 * u + 64, :]

    def share(e, total):
        psend[...] = total
        s = rcopy(psend, precv.at[e], p_s, p_r.at[e], partner)
        s.start()
        with jax.named_scope("share"):
            s.wait()
        y16[...] = (y16[...].astype(F32) + (psend[...] + precv[e])).astype(BF16)

    def row_split(first, n, x_of):
        for i in range(n):
            r_wait(first + i)
        return sum(jnp.dot(x_of(i), wr[first + i], preferred_element_type=F32) for i in range(n))

    def layer(l, carry):
        def gain_row(i):
            rows = gains[i].astype(F32)
            return jnp.where(l == 0, rows[0:1], rows[1:2])

        h[...] = rms(y16[...].astype(F32), gain_row(0))

        def project(first):
            tiles = []
            for i in range(first, first + NC):
                p_wait(i)
            for i in range(first, first + NC):
                r = jnp.dot(h[...], wp[i], preferred_element_type=F32).astype(BF16)
                tiles += [r[:, 128 * u:128 * u + 128] for u in range(CW // 128)]
            return tiles

        def k_copy(o):
            return rcopy(kvsend.at[ahead(o)], zkv.at[l, z, j], ak_s, ak_r.at[l], dev(z, ahead(o), 1 - c))

        def q_part(o):
            return rcopy(qsend.at[ahead(o) // 2], qa.at[l, j], aq_s, aq_r.at[l], dev(z, ahead(o), 1 - c))

        low = lax.broadcasted_iota(jnp.int32, (16, 128), 1) < 64
        with jax.named_scope("kv_proj"):
            ks = project(0)
            vs = project(NC)
            for u in range(NPAIR):
                k, v = ks[u].astype(F32), pltpu.roll(vs[u].astype(F32), 64, 1)
                kvsend[2 * u] = jnp.where(low, k, v).astype(BF16)
                kvsend[2 * u + 1] = jnp.where(low, v, k).astype(BF16)
        for o in (*offsets, 0):
            k_copy(o).start()
        with jax.named_scope("q_proj"):
            for u, q in enumerate(project(2 * NC)):
                qsend[u] = q
        for o in (*offsets, 0):
            q_part(o).start()
        for i in range(2 * g.reuse):
            p_load(l, GU + i)

        @pl.when(l == 0)
        def _():
            for k in range(2 * g.reuse, 3 * NC):
                p_load(1, k)

        @pl.when(l == 0)
        def _():
            kv_send(0, 1)
            w_wait(1)
            with jax.named_scope("kv"):
                for r in range(GROUPS):
                    keys_values(1, r)
            for i in range(2 * g.reuse, 2 * NF):
                p_load(0, GU + i)
            for i in range(NC, NF):
                r_load(0, DN + i)
        with jax.named_scope("a_wait"):
            wait_bytes(zkv.at[l, z], ak_r.at[l])

        def z_copy(dz):
            return rcopy(zkv.at[l, z], zkv.at[l, z], z_s.at[dz], z_r.at[l], dev(lax.rem(z + dz, NZ), j, c))

        for dz in (2, 1, 3):
            z_copy(dz).start()

        @pl.when(l == 0)
        def _():
            kv_send(0, 2)
            with jax.named_scope("relay0"):
                for turn, half in ((0, 0), (0, 1), (1, 0)):
                    kv_relay(0, turn, half)
        with jax.named_scope("z_wait"):
            wait_bytes(qa.at[l], aq_r.at[l])
            qm = jnp.where(mine, qa[l].reshape(COLS, 128).astype(F32), 0.0).astype(BF16)
            wait_bytes(zkv.at[l, pl.ds(0, NZ - 1)], z_r.at[l])

        row = z * COLS + lax.broadcasted_iota(jnp.int32, (COLS, COLS), 0)
        col = lax.broadcasted_iota(jnp.int32, (COLS, COLS), 1)
        with jax.named_scope("self_att"):
            scores = []
            for zz in range(NZ):
                s = lax.dot_general(qm, zkv[l, zz].reshape(COLS, 128), NT, preferred_element_type=F32) * SCALE2
                scores.append(jnp.where(zz * COLS + col <= row, s, NEG))
            top = functools.reduce(jnp.maximum, [jnp.max(s, axis=1, keepdims=True) for s in scores])
            den = jnp.zeros((COLS, 1), F32)
            num = jnp.zeros((COLS, 128), F32)
            for zz in range(NZ):
                e = jnp.exp2(scores[zz] - top)
                den = den + jnp.sum(e, axis=1, keepdims=True)
                num = num + jnp.dot(e.astype(BF16), zkv[l, zz].reshape(COLS, 128), preferred_element_type=F32)
            o_all = pltpu.roll(jnp.where(mine, 0.0, num / den), 64, 1).astype(BF16)
            osend[...] = o_all.reshape(NP, 16, 128)

        def o_copy(o):
            return rcopy(osend.at[ahead(o)], orecv.at[l, j], o_s, o_r.at[l], dev(z, ahead(o), 1 - c))

        for o in (*offsets, 0):
            o_copy(o).start()
        wait_bytes(kvsend, ak_s)
        wait_bytes(kvsend, aq_s)
        for dz in range(1, NZ):
            z_copy(dz).wait_send()

        @pl.when(l == 0)
        def _():
            with jax.named_scope("relay1"):
                kv_relay(0, 1, 1)
        with jax.named_scope("o_wait"):
            wait_bytes(orecv.at[l], o_r.at[l])

        for u in range(NPAIR):
            pair = orecv[l, 2 * u].astype(F32) + orecv[l, 2 * u + 1].astype(F32)
            xs[128 * u // CW, :, 128 * u % CW:128 * u % CW + 128] = pair.astype(BF16)
        with jax.named_scope("self_o"):
            total = row_split(0, NC, lambda i: xs[i])
        for i in range(NC):
            r_load(l, DN + i)
        wait_bytes(osend, o_s)
        share(l * 3, total)

        h[...] = rms(y16[...].astype(F32), gain_row(1))
        stack = []
        for i in range(NC):
            p_wait(3 * NC + i)
        for i in range(NC):
            r = jnp.dot(h[...], wp[3 * NC + i], preferred_element_type=F32).astype(BF16).astype(F32)
            stack += [r[:, 128 * u:128 * u + 128] for u in range(CW // 128)]
        turned = jnp.concatenate(stack, axis=0).T
        qts[...] = jnp.concatenate([turned[:64], turned[64:]], axis=1).astype(BF16)

        def q_copy(o):
            return rcopy(qts, qrecv.at[l, j], q_s, q_r.at[l, j], dev(z, ahead(o), 1 - c))

        for o in (*order, 0):
            q_copy(o).start()

        @pl.when(l == 0)
        def _():
            for k in range(3 * NC, 4 * NC):
                p_load(1, k)
            for stage in range(3):
                kv_send(1, stage)

        one = jnp.where(lax.broadcasted_iota(jnp.int32, (64, COLS), 0) == 0, 1.0, 0.0).astype(BF16)

        def tile_of(o):
            return ahead(offset_of(o))

        def q_spread(o, to):
            x = qrecv[l, tile_of(o)].astype(F32) * SCALE2
            hi = x.astype(BF16)
            x = x - hi.astype(F32)
            mid = x.astype(BF16)
            low = (x - mid.astype(F32)).astype(BF16)
            to[...] = jnp.concatenate([hi, mid, low, one], axis=0)

        def q_wait(o):
            ref = qrecv.at[l, tile_of(o)]
            pltpu.make_async_copy(ref, ref, q_r.at[l, tile_of(o)]).wait()

        with jax.named_scope("kv_wait"):
            kv_wait(l)
        with jax.named_scope("spread"):
            for blk in range(NB):
                spread(l, blk)

        CH = g.ch
        PER = 2 * TM // CH
        CHUNKS = NB * PER

        def score(queries, k):
            part = jnp.dot(kx[k // PER, k % PER * CH:k % PER * CH + CH, :], queries[...], preferred_element_type=F32)
            sbuf[k % NBUF][...] = part
            mbuf[k % NBUF][...] = jnp.max(part.reshape(CH // 16, 16, COLS), axis=0)

        def r_copy(o):
            to = tile_of(o)
            return rcopy(acc.at[to], rrecv.at[l, j], r_s, r_r.at[l], dev(z, to, 1 - c))

        def attend(i, queries, following):
            num = jnp.zeros((64, COLS), F32)
            den = jnp.zeros((8, COLS), F32)
            top = jnp.full((1, COLS), -3e38, F32)
            for k in range(CHUNKS):
                if k + LAG < CHUNKS:
                    score(queries, k + LAG)
                elif following is not None:
                    score(following, k + LAG - CHUNKS)
                new = jnp.maximum(jnp.max(mbuf[k % NBUF][...], axis=0, keepdims=True), top)
                old = jnp.exp2(top - new)
                e = jnp.exp2(sbuf[k % NBUF][...] - new)
                den = den * old + jnp.sum(e.reshape(CH // 8, 8, COLS), axis=0)
                v = vx[k // PER, :, k % PER * CH:k % PER * CH + CH]
                num = num * old + jnp.dot(v, e.astype(BF16), preferred_element_type=F32)
                top = new
            den = jnp.sum(den, axis=0, keepdims=True)
            for half in range(2):
                cut = slice(half * HC, half * HC + HC)
                acc[i, 64 * half:64 * half + 64] = num[:, cut]
                acc[i, 128 + half:129 + half] = top[:, cut]
                acc[i, 130 + half:131 + half] = den[:, cut]

        with jax.named_scope("q_wait"):
            q_wait(0)
        q_spread(0, qxa)
        for k in range(LAG):
            score(qxa, k)

        def tiles(p):
            o = 2 * p
            q_wait(o + 1)
            q_wait(o + 2)
            q_spread(o + 1, qxb)
            attend(tile_of(o), qxa, qxb)
            q_spread(o + 2, qxa)
            attend(tile_of(o + 1), qxb, qxa)
            r_copy(o).start()
            r_copy(o + 1).start()

        with jax.named_scope("tiles"):
            loop(NP // 2 - 1, tiles)
            q_wait(NP - 1)
            q_spread(NP - 1, qxb)
            attend(tile_of(NP - 2), qxa, qxb)
            r_copy(NP - 2).start()
            attend(j, qxb, None)
            r_copy(NP - 1).start()
        @pl.when(l == 0)
        def _():
            for turn in range(2):
                for half in range(2):
                    kv_relay(1, turn, half)
        wait_bytes(qrecv.at[l], q_s)

        with jax.named_scope("r_wait"):
            wait_bytes(rrecv.at[l], r_r.at[l])
        parts = []
        for half in range(2):
            top = functools.reduce(jnp.maximum, [rrecv[l, i, 128 + half:129 + half] for i in range(NP)])
            num = jnp.zeros((64, HC), F32)
            den = jnp.zeros((1, HC), F32)
            for i in range(NP):
                w = jnp.exp2(rrecv[l, i, 128 + half:129 + half] - top)
                num = num + rrecv[l, i, 64 * half:64 * half + 64] * w
                den = den + rrecv[l, i, 130 + half:131 + half] * w
            parts.append(num / den)
        turned = jnp.concatenate(parts, axis=0).T.astype(BF16)
        for u in range(NPAIR):
            xs[128 * u // CW, :, 128 * u % CW:128 * u % CW + 128] = turned[16 * u:16 * u + 16]
        wait_bytes(acc, r_s)
        with jax.named_scope("cross_o"):
            total = row_split(NC, NC, lambda i: xs[i])

        @pl.when(l == 0)
        def _():
            for k in range(NC, 2 * NC):
                r_load(1, k)
        share(l * 3 + 1, total)

        h[...] = rms(y16[...].astype(F32), gain_row(2))

        def gate_up(i):
            slot = 2 * i if i < g.reuse else 4 * NC + 2 * (i - g.reuse)
            a = jnp.dot(h[...], wp[slot], preferred_element_type=F32)
            b = jnp.dot(h[...], wp[slot + 1], preferred_element_type=F32)
            act[i] = (a / (1.0 + jnp.exp(-a)) * b).astype(BF16)

        with jax.named_scope("gate_up"):
            for i in (*range(2 * g.reuse), *range(4 * NC, g.pslots)):
                p_wait(i)
            for i in range(NF):
                gate_up(i)

        @pl.when(l == 0)
        def _():
            for k in range(2 * g.reuse):
                p_load(1, k)

        @pl.when(l == 0)
        def _():
            for i in range(2 * g.reuse, 2 * NF):
                p_load(1, GU + i)

        with jax.named_scope("down"):
            slots = [i if i < NC else NC + i for i in range(NF)]
            for slot in slots:
                r_wait(slot)
            total = sum(jnp.dot(act[i], wr[slot], preferred_element_type=F32) for i, slot in enumerate(slots))

        @pl.when(l == 0)
        def _():
            for k in range(NC):
                r_load(1, k)
            for i in range(NC, NF):
                r_load(1, DN + i)
        share(l * 3 + 2, total)
        return carry

    lax.fori_loop(0, LAYERS, layer, 0)
    for n in range(LAYERS):
        kv_sent(n)
        kv_relayed(n)
    y = y16[...].astype(F32)
    out_ref[...] = jnp.where(c == 0, y[0:8], y[8:16]).astype(BF16)


def solution(mesh):
    n = mesh.shape["sp"]
    row_spec = P(("dp", "sp"), None)

    def device_fn(dec_hidden, memory, mem_len, gain_self, gain_cross, gain_mlp, self_q, self_k, self_v, self_o, cross_q, cross_k, cross_v, cross_o, mlp_gate, mlp_up, mlp_down):
        tm, d_model = memory.shape
        args = (mem_len, dec_hidden, memory, cross_k, cross_v, gain_self, gain_cross, gain_mlp, self_q, self_k, self_v, self_o, cross_q, cross_o, mlp_gate, mlp_up, mlp_down)

        def run(nb):
            g = Geo(n, d_model, mlp_gate.shape[-1], tm, nb)
            return functools.partial(call, g)

        nz, chips = GEOMETRY[n]
        return lax.cond(mem_len[0] <= 2 * 2 * chips * tm, run(2), run(3), *args)

    def call(g, *args):
        NP, NZ, NB, COLS, CW, NC, NF, D = g.np_, g.nz, g.nb, g.cols, g.cw, g.nc, g.nf, g.d
        tm = g.tm
        vmem = pl.BlockSpec(memory_space=pltpu.VMEM)
        hbm = pl.BlockSpec(memory_space=pl.ANY)
        dma = pltpu.SemaphoreType.DMA
        scratch = [
            pltpu.SMEM((1,), jnp.int32),
            pltpu.VMEM((2, 8, D), BF16),
            pltpu.VMEM((16, D), BF16),
            pltpu.VMEM((16, D), BF16),
            pltpu.VMEM((3, LAYERS, D), BF16),
            pltpu.VMEM((g.pslots, D, CW), BF16),
            pltpu.VMEM((g.rslots, CW, D), BF16),
            pltpu.VMEM((NP, 16, 128), BF16),
            pltpu.VMEM((g.npair, 16, 128), BF16),
            pltpu.VMEM((LAYERS, NP, 16, 128), BF16),
            pltpu.VMEM((LAYERS, NZ, NP, 16, 128), BF16),
            pltpu.VMEM((NP, 16, 128), BF16),
            pltpu.VMEM((LAYERS, NP, 16, 128), BF16),
            pltpu.VMEM((NC, 16, CW), BF16),
            pltpu.VMEM((16, D), F32),
            pltpu.VMEM((3 * LAYERS, 16, D), F32),
            pltpu.VMEM((64, COLS), BF16),
            pltpu.VMEM((LAYERS, NP, 64, COLS), BF16),
            pltpu.VMEM((LAYERS, 2, tm, 128), BF16),
            pltpu.VMEM((LAYERS, NB, 2, tm, 128), BF16),
            pltpu.VMEM((NB, 2 * tm, 256), BF16),
            pltpu.VMEM((NB, 64, 2 * tm), BF16),
            pltpu.VMEM((256, COLS), BF16),
            pltpu.VMEM((256, COLS), BF16),
            pltpu.VMEM((NP, 136, COLS // 2), F32),
            pltpu.VMEM((LAYERS, NP, 136, COLS // 2), F32),
            pltpu.VMEM((NF, 16, CW), BF16),
            *[pltpu.VMEM((g.ch, COLS), F32)] * NBUF,
            *[pltpu.VMEM((16, COLS), F32)] * NBUF,
            dma((g.pslots,)), dma((g.rslots,)), dma((5,)),
            dma(()), dma((LAYERS,)), dma(()), dma((LAYERS,)),
            dma((NZ,)), dma((LAYERS,)),
            dma(()), dma((LAYERS,)),
            dma(()), dma((3 * LAYERS,)),
            dma(()), dma((LAYERS, NP)),
            dma((LAYERS, 5, 2)), dma((LAYERS, NB, 2, 2)), dma((LAYERS, 2, 2, 2)),
            dma(()), dma((LAYERS,)), dma((min(2, tm // 256) + LAYERS,)),
        ]
        return pl.pallas_call(
            functools.partial(kernel, g),
            out_shape=jax.ShapeDtypeStruct(args[1].shape, BF16),
            in_specs=[hbm] * 17,
            out_specs=vmem,
            scratch_shapes=scratch,
            compiler_params=pltpu.CompilerParams(collective_id=0, has_side_effects=True, vmem_limit_bytes=67043328, flags=FLAGS),
            name=f"decoder{NB}",
        )(*args)

    return jax.shard_map(device_fn, mesh=mesh, in_specs=(row_spec, row_spec, P("dp")) + (P(),) * 14, out_specs=row_spec, check_vma=False)
```
